32 devices in a mesh: data: 2 (over x), expert: 16 (over z, y, core).
Axes of the slice: x: 2, y: 2, z: 4, core: 2. Of those that a mesh axis runs over, the one named last changes fastest.
Arguments:
- x: bfloat16 [2048, 2048], P(('data', 'expert')), parts along dimension 0
- idx: int32 [2048, 8], P(('data', 'expert')), parts along dimension 0
- g: float32 [2048, 8], P(('data', 'expert')), parts along dimension 0
- hot_tok: int32 [1024], P(('data', 'expert')), parts along dimension 0
- W1: bfloat16 [64, 2048, 1024], P('expert')
- W3: bfloat16 [64, 2048, 1024], P('expert')
- W2: bfloat16 [64, 1024, 2048], P('expert')
Outputs:
- output: bfloat16 [2048, 2048], P(('data', 'expert')), parts along dimension 0
There are 2 independent parts. The reference program is written for one: setup_inputs(seed, part) draws one part's arguments, and reference() takes and returns one part's arrays. A program takes and returns all parts, laid end to end along the dimension named above; an argument that names none is the same for every part.
All inputs are finite; a program needn't handle non-finite values.
Results may differ from the reference program's by a relative error of at most 0.001.
Values are sent between devices in bfloat16 or wider.
A program may use at most 1 GiB of HBM per device.

```python
import jax
import jax.numpy as jnp
from jax import lax

EXPERTS = 64
TOP = 8
D = 2048
FF = 1024
TOKENS = 64
HOT_DIV = 2
GROUP = 16

HOT_CAP = TOKENS // HOT_DIV
COLD_CAP = 2 * ((TOKENS * TOP - HOT_CAP + EXPERTS - 2) // (EXPERTS - 1))


def _weights(key, e, fan_in, fan_out):
    keys = jax.random.split(key, e)
    return lax.map(lambda k: (jax.random.normal(k, (fan_in, fan_out), jnp.float32) * fan_in ** -0.5).astype(jnp.bfloat16), keys)


def _chip_ids(key):
    k1, k2, k3 = jax.random.split(key, 3)
    t = jnp.arange(TOKENS)[:, None]
    j = jnp.arange(TOP)[None, :]
    hot = (t < HOT_CAP) & (j == 0)
    c = jnp.where(t < HOT_CAP, t * (TOP - 1) + j - 1, HOT_CAP * (TOP - 1) + (t - HOT_CAP) * TOP + j)
    seq = jnp.concatenate([jnp.arange(EXPERTS - 1), jnp.arange((EXPERTS - 1) // 2)])
    m = EXPERTS - 1 + (EXPERTS - 1) // 2
    off = jax.random.randint(k1, (), 0, m)
    perm = jax.random.permutation(k2, EXPERTS - 1)
    ids = jnp.flip(jnp.where(hot, 0, 1 + perm[seq[(c + off) % m]]), axis=1)
    shift = jax.random.randint(k3, (), 0, TOKENS)
    ids = jnp.roll(ids, shift, axis=0)
    hot_tok = jnp.sort((jnp.arange(HOT_CAP) + shift) % TOKENS)
    return ids.astype(jnp.int32), hot_tok.astype(jnp.int32)


def setup_inputs(seed: int = 0, part: int = 0) -> dict:
    kdata, kw = jax.random.split(jax.random.PRNGKey(seed))
    kx, kr, kg = jax.random.split(jax.random.fold_in(kdata, part), 3)
    k1, k3, k2 = jax.random.split(kw, 3)
    x = jax.random.normal(kx, (GROUP * TOKENS, D), jnp.float32).astype(jnp.bfloat16)
    ids, hot = jax.vmap(_chip_ids)(jax.random.split(jax.random.fold_in(kr, 7), GROUP))
    idx = ids.reshape(GROUP * TOKENS, TOP)
    u = jax.random.uniform(kg, (GROUP * TOKENS, TOP), jnp.float32)
    g = jnp.where(idx == 0, 0.6 + 0.4 * u, 0.2 + 0.5 * u)
    return {
        'x': x,
        'idx': idx,
        'g': g,
        'hot_tok': hot.reshape(GROUP * HOT_CAP),
        'W1': _weights(k1, EXPERTS, D, FF),
        'W3': _weights(k3, EXPERTS, D, FF),
        'W2': _weights(k2, EXPERTS, FF, D),
    }


def _expert(xr, w1, w3, w2):
    a = jnp.dot(xr, w1, preferred_element_type=jnp.float32)
    b = jnp.dot(xr, w3, preferred_element_type=jnp.float32)
    u = (jax.nn.silu(a) * b).astype(jnp.bfloat16)
    return jnp.dot(u, w2, preferred_element_type=jnp.float32).astype(jnp.bfloat16)


def reference(x, idx, g, hot_tok, W1, W3, W2):
    gate = jnp.where(idx == 0, g, 0.0).sum(axis=1)
    rows = (jnp.arange(GROUP)[:, None] * TOKENS + hot_tok.reshape(GROUP, HOT_CAP)).reshape(-1)
    hh = _expert(x[rows], W1[0], W3[0], W2[0]).astype(jnp.float32)
    y = jnp.zeros((GROUP * TOKENS, D), jnp.float32).at[rows].add(gate[rows][:, None] * hh)
    flat = idx.reshape(-1)
    order = jnp.argsort(flat, stable=True)
    counts = jnp.bincount(flat, length=EXPERTS)
    starts = jnp.cumsum(counts) - counts
    cap = GROUP * COLD_CAP
    order = jnp.concatenate([order, jnp.zeros((cap,), order.dtype)])
    gflat = g.reshape(-1)

    def step(y, ew):
        e, w1, w3, w2 = ew
        r = lax.dynamic_slice(order, (starts[e],), (cap,))
        valid = jnp.arange(cap) < counts[e]
        he = _expert(x[r // TOP], w1, w3, w2).astype(jnp.float32)
        return y.at[r // TOP].add(jnp.where(valid[:, None], gflat[r][:, None] * he, 0.0)), None

    y, _ = lax.scan(step, y, (jnp.arange(1, EXPERTS), W1[1:], W3[1:], W2[1:]))
    return y.astype(jnp.bfloat16)
```

```python
import jax
import jax.numpy as jnp
from jax import lax
from jax.sharding import PartitionSpec as P


def _pieces(g):
    hi = lax.reduce_precision(g, 8, 7)
    mid = lax.reduce_precision(g - hi, 8, 7)
    lo = g - hi - mid
    return hi.astype(jnp.bfloat16), mid.astype(jnp.bfloat16), lo.astype(jnp.bfloat16)


def _expert(xs, w1, w3, w2):
    a = jnp.dot(xs, w1, preferred_element_type=jnp.float32)
    b = jnp.dot(xs, w3, preferred_element_type=jnp.float32)
    u = (jax.nn.silu(a) * b).astype(jnp.bfloat16)
    return jnp.dot(u, w2, preferred_element_type=jnp.float32).astype(jnp.bfloat16)


def solution(mesh):
    n = mesh.shape['expert']

    def local(x, idx, g, hot_tok, w1, w3, w2):
        t, d = x.shape
        k = idx.shape[1]
        el = w1.shape[0]
        e = el * n
        ch = hot_tok.shape[0]
        cap = 2 * ((t * k - ch + e - 2) // (e - 1))
        me = lax.axis_index('expert')
        meta = jnp.concatenate([idx.astype(jnp.float32).T, g.T], axis=0)
        meta = lax.all_gather(meta, 'expert', axis=0)
        xall = lax.all_gather(x, 'expert', axis=0)
        ids, gs = meta[:, :k], meta[:, k:]
        mine = (me * el + jnp.arange(el)).astype(jnp.float32)
        eq = ids[:, None] == mine[None, :, None, None]
        gate = jnp.where(eq, gs[:, None], 0.0).sum(axis=2)
        hit = eq.any(axis=2)
        tri = (jnp.arange(t)[:, None] < jnp.arange(t)[None, :]).astype(jnp.bfloat16)
        rank = jnp.dot(hit.astype(jnp.bfloat16), tri, preferred_element_type=jnp.float32)
        rank = jnp.where(hit, rank, -1.0)
        sizes = [ch] + [cap] * (el - 1)
        offs = [sum(sizes[:i]) for i in range(el)]
        oh = jnp.concatenate([rank[:, i, None, :] == jnp.arange(sizes[i], dtype=jnp.float32)[None, :, None] for i in range(el)], axis=1)
        gg = jnp.concatenate([jnp.broadcast_to(gate[:, i, None, :], (n, sizes[i], t)) for i in range(el)], axis=1)
        gg = jnp.where(oh, gg, 0.0)
        xs = jnp.einsum('nst,ntd->nsd', oh.astype(jnp.bfloat16), xall, preferred_element_type=jnp.float32).astype(jnp.bfloat16)
        hs = []
        for i in range(el):
            xe = xs[:, offs[i]:offs[i] + sizes[i]].reshape(n * sizes[i], d)
            hs.append(_expert(xe, w1[i], w3[i], w2[i]).reshape(n, sizes[i], d))
        h = jnp.concatenate(hs, axis=1)
        g3 = jnp.concatenate(_pieces(gg), axis=1)
        h3 = jnp.concatenate([h, h, h], axis=1)
        part = jnp.einsum('nst,nsd->ntd', g3, h3, preferred_element_type=jnp.float32)
        y = lax.psum_scatter(part.reshape(n * t, d), 'expert', scatter_dimension=0, tiled=True)
        return y.astype(jnp.bfloat16)

    rows = P(('data', 'expert'))
    wspec = P('expert')
    return jax.shard_map(local, mesh=mesh, in_specs=(rows, rows, rows, rows, wspec, wspec, wspec), out_specs=rows, check_vma=False)
```

```python
import functools

import jax
import jax.numpy as jnp
from jax import lax
from jax.experimental import pallas as pl
from jax.experimental.pallas import tpu as pltpu
from jax.sharding import PartitionSpec as P

F32, BF16 = jnp.float32, jnp.bfloat16
RELS = (0, 1, 7, 2, 6, 3, 5, 4)
SLOT = {r: i for i, r in enumerate(RELS)}
R, L = 0, 1


def _kernel(nch, ch, cap, nz, x_hbm, meta_ref, w1, w3, w2, out_ref,
            X, M, W, XG, U, OH, GT, OWN, SIB, S, RR,
            xs, wsem, ags, agr, ms, mr, ss, sr, ds_, dr, rs, rr):
    T, D = x_hbm.shape
    el, F = w1.shape[0], w1.shape[2]
    DC = D // nch
    HC = DC // 2
    KH = D // 2
    NT = min(256, F)
    k = meta_ref.shape[0] // 2
    caps = [ch] + [cap] * (el - 1)
    offs = [2 * sum(caps[:i]) for i in range(el)]
    rows = 2 * sum(caps)

    idx = lax.axis_index('expert')
    core = idx % 2
    chip = idx // 2
    cz, cy = chip // 2, chip % 2
    pos = cz * (1 - cy) + (2 * nz - 1 - cz) * cy

    def device(p):
        y = p // nz
        z = p * (1 - y) + (2 * nz - 1 - p) * y
        return (z * 2 + y) * 2 + core

    right = device((pos + 1) % (2 * nz))
    left = device((pos + 2 * nz - 1) % (2 * nz))
    side = chip * 2 + 1 - core
    dev = (right, left)

    def remote(src, dst, s_sem, r_sem, who):
        return pltpu.make_async_remote_copy(src_ref=src, dst_ref=dst, send_sem=s_sem, recv_sem=r_sem,
                                            device_id={'expert': who}, device_id_type=pl.DeviceIdType.MESH)

    wloads = []
    for e in range(el):
        for j, w in enumerate((w1, w1, w3, w3)):
            wloads.append(pltpu.make_async_copy(w.at[e, pl.ds((j % 2) * KH, KH), :], W.at[4 * e + j], wsem.at[4 * e + j]))
    xloads = [pltpu.make_async_copy(x_hbm.at[:, pl.ds(c * DC, DC)], X.at[c, pl.ds(0, T), :], xs.at[c]) for c in range(nch)]
    for c in xloads:
        c.start()
    for c in wloads:
        c.start()
    M[0] = meta_ref[...]

    barrier = pltpu.get_barrier_semaphore()
    for who in (right, left, side):
        pl.semaphore_signal(barrier, inc=1, device_id={'expert': who}, device_id_type=pl.DeviceIdType.MESH)
    pl.semaphore_wait(barrier, 3)

    hc = nch // 2

    def blk(rel, s, hf):
        return X.at[pl.ds(hf * hc, hc), pl.ds(SLOT[rel] * 2 * T + s * T, T), :]

    def has(d, s, hf):
        return s <= 3 or (s == 4 and hf == d)

    def ag(d, s, hf):
        a, b = ((1 - s) % 8, -s % 8) if d == R else (s - 1, s)
        return remote(blk(a, 0, hf), blk(b, 0, hf), ags.at[d, s - 1, hf], agr.at[d, s - 1, hf], dev[d])

    def hasm(d, s):
        return s <= 3 or (s == 4 and d == R)

    def agm(d, s):
        a, b = ((1 - s) % 8, -s % 8) if d == R else (s - 1, s)
        return remote(M.at[2 * SLOT[a]], M.at[2 * SLOT[b]], ms.at[d, s - 1], mr.at[d, s - 1], dev[d])

    def sd(rel, hf):
        return remote(blk(rel, 0, hf), blk(rel, 1, hf), ss.at[rel, hf], sr.at[rel, hf], side)

    def sdm(rel):
        return remote(M.at[2 * SLOT[rel]], M.at[2 * SLOT[rel] + 1], ss.at[rel, 2], sr.at[rel, 2], side)

    sent = []

    def go(c):
        c.start()
        sent.append(c)

    for c in xloads:
        c.wait()
    for d in (R, L):
        go(agm(d, 1))
    for hf in range(2):
        for d in (R, L):
            go(ag(d, 1, hf))
    go(sdm(0))
    for hf in range(2):
        go(sd(0, hf))

    def advance(s, hf):
        if hf == 0:
            for d in (R, L):
                if hasm(d, s):
                    agm(d, s).wait_recv()
                    if hasm(d, s + 1) and s < 4:
                        go(agm(d, s + 1))
                    go(sdm(-s % 8 if d == R else s))
        for d in (R, L):
            if has(d, s, hf):
                ag(d, s, hf).wait_recv()
                if s < 4 and has(d, s + 1, hf):
                    go(ag(d, s + 1, hf))
                go(sd(-s % 8 if d == R else s, hf))

    tr = lax.broadcasted_iota(jnp.int32, (2 * T, 2 * T), 0)
    tc = lax.broadcasted_iota(jnp.int32, (2 * T, 2 * T), 1)
    tri = jnp.where((tr < tc) & (tr // T == tc // T), 1.0, 0.0).astype(BF16)

    def prep(slot):
        m = M[2 * slot] + pltpu.roll(M[2 * slot + 1], T, 1)
        ids, gs = m[:k], m[k:]
        hits, gates = [], []
        for le in range(el):
            eq = ids == (idx * el + le).astype(F32)
            hits.append(jnp.max(jnp.where(eq, 1.0, 0.0), axis=0, keepdims=True))
            gates.append(jnp.sum(jnp.where(eq, gs, 0.0), axis=0, keepdims=True))
        hm = jnp.concatenate(hits + [jnp.zeros((16 - el, 2 * T), F32)], axis=0)
        rank = jnp.dot(hm.astype(BF16), tri, preferred_element_type=F32)
        lane = lax.broadcasted_iota(jnp.int32, (1, 2 * T), 1)
        oh, gg = [], []
        for le in range(el):
            key = jnp.where(hits[le] > 0.0, rank[le:le + 1] + jnp.where(lane >= T, float(caps[le]), 0.0), -1.0)
            hit = lax.broadcasted_iota(jnp.int32, (2 * caps[le], 2 * T), 0).astype(F32) == key
            oh.append(jnp.where(hit, 1.0, 0.0))
            gg.append(jnp.where(hit, gates[le], 0.0))
        OH[slot] = jnp.concatenate(oh, axis=0).astype(BF16)
        gv = jnp.concatenate(gg, axis=0)
        hi = gv.astype(BF16).astype(F32)
        mid = (gv - hi).astype(BF16).astype(F32)
        lo = gv - hi - mid
        GT[slot] = jnp.concatenate([hi, mid, lo], axis=0).T.astype(BF16)

    def arrive(g):
        for rel in RELS[4 * g:4 * g + 4]:
            for hf in range(2):
                sd(rel, hf).wait_recv()
            sdm(rel).wait_recv()

    def gather(g):
        def body(i, _):
            slot = 4 * g + i
            prep(slot)
            for c in range(nch):
                v = jnp.dot(OH[slot], X[c, pl.ds(pl.multiple_of(slot * 2 * T, 2 * T), 2 * T), :], preferred_element_type=F32).astype(BF16)
                for le in range(el):
                    n2 = 2 * caps[le]
                    XG[pl.ds(pl.multiple_of(4 * offs[le] + i * n2, 16), n2), c * DC:(c + 1) * DC] = v[offs[le]:offs[le] + n2]
            return 0
        lax.fori_loop(0, 4, body, 0)

    def expert(e, g):
        m = 8 * caps[e]
        src = pl.ds(4 * offs[e], m)
        dst = pl.ds(8 * offs[e] + g * m, m)

        def body(n, _):
            cols = pl.ds(pl.multiple_of(n * NT, NT), NT)
            xa, xb = XG[src, :KH], XG[src, KH:]
            a = jnp.dot(xa, W[4 * e, :, cols], preferred_element_type=F32) + jnp.dot(xb, W[4 * e + 1, :, cols], preferred_element_type=F32)
            b = jnp.dot(xa, W[4 * e + 2, :, cols], preferred_element_type=F32) + jnp.dot(xb, W[4 * e + 3, :, cols], preferred_element_type=F32)
            U[dst, cols] = (a * jax.nn.sigmoid(a) * b).astype(BF16)
            return 0
        lax.fori_loop(0, F // NT, body, 0)

    def loaded(e):
        for c in wloads[4 * e:4 * e + 4]:
            c.wait()

    for s in (1, 2):
        for hf in range(2):
            advance(s, hf)
    arrive(0)
    gather(0)
    loaded(0)
    expert(0, 0)
    advance(3, 0)
    loaded(1)
    expert(1, 0)
    advance(3, 1)
    loaded(2)
    expert(2, 0)
    loaded(3)
    expert(3, 0)
    advance(4, 0)
    advance(4, 1)
    arrive(1)
    gather(1)
    w2loads = []
    for e in range(el):
        expert(e, 1)
        if e < 2:
            for j in range(el):
                c = pltpu.make_async_copy(w2.at[j, :, pl.ds(e * KH, KH)], W.at[4 * e + j], wsem.at[4 * e + j])
                c.start()
                w2loads.append(c)
    for c in sent:
        c.wait_send()
    del sent[:]

    def h_rows(slot, lo, n):
        return X.at[slot // 2, pl.ds((slot % 2) * 3 * rows + lo, n), :]

    NF = 5

    def d2d(c, part):
        sl = pl.ds(NF, 8 - NF) if part == 0 else pl.ds(0, NF)
        return remote(SIB.at[c % 2, sl], S.at[c, sl], ds_.at[c, part], dr.at[c, part], side)

    def tile(c):
        hf, off = c // 2, (c % 2) * DC
        if off == 0:
            for w in w2loads[4 * hf:4 * hf + 4]:
                w.wait()
        if c >= 2:
            for part in range(2):
                d2d(c - 2, part).wait_send()
        nt = min(256, DC)
        for e in range(el):
            m = 16 * caps[e]
            n2 = 2 * caps[e]
            for n in range(DC // nt):
                h = jnp.dot(U[pl.ds(8 * offs[e], m), :], W[4 * hf + e, :, pl.ds(off + n * nt, nt)], preferred_element_type=F32).astype(BF16)
                for slot in range(8):
                    for p in range(3):
                        h_rows(slot, p * rows + offs[e], n2)[:, n * nt:(n + 1) * nt] = h[slot * n2:(slot + 1) * n2]
        for part in range(2):
            lo, hi = (NF, 8) if part == 0 else (0, NF)

            def body(slot, _):
                src = pl.ds(pl.multiple_of((slot % 2) * 3 * rows, 16), 3 * rows)
                v = jnp.dot(GT[slot], X[slot // 2, src, :], preferred_element_type=F32)
                OWN[c, slot] = v[:T]
                SIB[c % 2, slot] = v[T:]
                return 0
            lax.fori_loop(lo, hi, body, 0)
            d2d(c, part).start()

    A, B = slice(0, HC), slice(HC, DC)

    def ring(c, s, d):
        cols = pl.ds(0, DC) if s else pl.ds(d * HC, HC)
        rel = 4 - s if d == R else 4 + s
        return remote(OWN.at[c, SLOT[rel], :, cols], RR.at[c, d, s, :, cols], rs.at[c, d, s], rr.at[c, d, s], dev[d])

    def step(c, s):
        if s == 0:
            d2d(c, 0).wait_recv()
            OWN[c, SLOT[4]] += S[c, SLOT[4]]
        if s == 2:
            d2d(c, 1).wait_recv()
        for d in (R, L):
            if s:
                q = SLOT[4 - s if d == R else 4 + s]
                ring(c, s - 1, d).wait_recv()
                if s == 1:
                    h, o = (A, B) if d == R else (B, A)
                    OWN[c, q, :, h] += S[c, q, :, h] + RR[c, d, 0, :, h]
                    OWN[c, q, :, o] += S[c, q, :, o]
                else:
                    OWN[c, q] += S[c, q] + RR[c, d, s - 1]
            go(ring(c, s, d))

    def final(c):
        for d in (R, L):
            ring(c, 3, d).wait_recv()
        y = OWN[c, 0] + S[c, 0] + (RR[c, R, 3] + RR[c, L, 3])
        out_ref[:, c * DC:(c + 1) * DC] = y.astype(BF16)

    tile(0)
    tile(1)
    step(0, 0)
    tile(2)
    step(1, 0)
    step(0, 1)
    tile(3)
    step(2, 0)
    step(1, 1)
    step(0, 2)
    step(3, 0)
    step(2, 1)
    step(1, 2)
    step(0, 3)
    step(3, 1)
    step(2, 2)
    step(1, 3)
    final(0)
    step(3, 2)
    step(2, 3)
    final(1)
    step(3, 3)
    final(2)
    final(3)
    for c in sent:
        c.wait_send()
    for c in (2, 3):
        for part in range(2):
            d2d(c, part).wait_send()


def solution(mesh):
    n = mesh.shape['expert']
    nz = n // 4

    def local(x, idx, g, hot_tok, w1, w3, w2):
        t, d = x.shape
        k = idx.shape[1]
        el, _, f = w1.shape
        e = el * n
        ch = hot_tok.shape[0]
        cap = 2 * ((t * k - ch + e - 2) // (e - 1))
        nch = 4
        dc = d // nch
        rows = 2 * (ch + (el - 1) * cap)
        meta = jnp.concatenate([idx.astype(F32).T, g.T], axis=0)
        meta = jnp.pad(meta, ((0, 0), (0, t)))
        dma = pltpu.SemaphoreType.DMA
        vmem = pl.BlockSpec(memory_space=pltpu.VMEM)
        hbm = pl.BlockSpec(memory_space=pl.ANY)
        return pl.pallas_call(
            functools.partial(_kernel, nch, ch, cap, nz),
            name='moe',
            out_shape=jax.ShapeDtypeStruct((t, d), BF16),
            in_specs=[hbm, vmem, hbm, hbm, hbm],
            out_specs=vmem,
            scratch_shapes=[
                pltpu.VMEM((nch, 16 * t, dc), BF16),
                pltpu.VMEM((16, 2 * k, 2 * t), F32),
                pltpu.VMEM((4 * el, d // 2, f), BF16),
                pltpu.VMEM((4 * rows, d), BF16),
                pltpu.VMEM((8 * rows, f), BF16),
                pltpu.VMEM((8, rows, 2 * t), BF16),
                pltpu.VMEM((8, 2 * t, 3 * rows), BF16),
                pltpu.VMEM((nch, 8, t, dc), F32),
                pltpu.VMEM((2, 8, t, dc), F32),
                pltpu.VMEM((nch, 8, t, dc), F32),
                pltpu.VMEM((nch, 2, 4, t, dc), F32),
                dma((nch,)), dma((4 * el,)),
                dma((2, 4, 2)), dma((2, 4, 2)), dma((2, 4)), dma((2, 4)),
                dma((8, 3)), dma((8, 3)), dma((nch, 2)), dma((nch, 2)),
                dma((nch, 2, 4)), dma((nch, 2, 4)),
            ],
            compiler_params=pltpu.CompilerParams(collective_id=0, has_side_effects=True, vmem_limit_bytes=67043328),
        )(x, meta, w1, w3, w2)

    rows = P(('data', 'expert'))
    wspec = P('expert')
    return jax.shard_map(local, mesh=mesh, in_specs=(rows, rows, rows, rows, wspec, wspec, wspec), out_specs=rows, check_vma=False)
```

```python
import functools

import jax
import jax.numpy as jnp
from jax import lax
from jax.experimental import pallas as pl
from jax.experimental.pallas import tpu as pltpu
from jax.sharding import PartitionSpec as P

F32, BF16 = jnp.float32, jnp.bfloat16
RELS = (0, 1, 7, 2, 6, 3, 5, 4)
SLOT = {r: i for i, r in enumerate(RELS)}
R, L = 0, 1


def _kernel(nch, ch, cap, nz, x_hbm, ids_ref, g_ref, w1, w3, w2, out_ref,
            X, M, W, V, XG, U, OH, GT, OWN, SF, SN, S, RR,
            xs, wsem, vsem, ags, agr, ms, mr, ss, sr, ds_, dr, rs, rr):
    T, D = x_hbm.shape
    el, F = w1.shape[0], w1.shape[2]
    DC = D // nch
    HC = DC // 2
    KH = D // 2
    NT = min(256, F)
    k = ids_ref.shape[0]
    caps = [ch] + [cap] * (el - 1)
    offs = [2 * sum(caps[:i]) for i in range(el)]
    rows = 2 * sum(caps)

    idx = lax.axis_index('expert')
    core = idx % 2
    chip = idx // 2
    cz, cy = chip // 2, chip % 2
    pos = cz * (1 - cy) + (2 * nz - 1 - cz) * cy

    def device(p):
        y = p // nz
        z = p * (1 - y) + (2 * nz - 1 - p) * y
        return (z * 2 + y) * 2 + core

    right = device((pos + 1) % (2 * nz))
    left = device((pos + 2 * nz - 1) % (2 * nz))
    side = chip * 2 + 1 - core
    dev = (right, left)

    def remote(src, dst, s_sem, r_sem, who):
        return pltpu.make_async_remote_copy(src_ref=src, dst_ref=dst, send_sem=s_sem, recv_sem=r_sem,
                                            device_id={'expert': who}, device_id_type=pl.DeviceIdType.MESH)

    xloads = [pltpu.make_async_copy(x_hbm.at[:, pl.ds(c * DC, DC)], X.at[c, pl.ds(0, T), :], xs.at[c]) for c in range(nch)]
    for c in xloads:
        c.start()
    M[0, :k, :T] = ids_ref[...].astype(F32)
    M[0, k:, :T] = g_ref[...]
    M[0, :, T:] = jnp.zeros((2 * k, T), F32)

    barrier = pltpu.get_barrier_semaphore()
    for who in (right, left, side):
        pl.semaphore_signal(barrier, inc=1, device_id={'expert': who}, device_id_type=pl.DeviceIdType.MESH)
    wloads = []
    for e in range(el):
        for j, w in enumerate((w1, w1, w3, w3)):
            wloads.append(pltpu.make_async_copy(w.at[e, pl.ds((j % 2) * KH, KH), :], W.at[4 * e + j], wsem.at[4 * e + j]))
    vloads = [pltpu.make_async_copy(w2.at[e, :, pl.ds(0, DC)], V.at[e], vsem.at[0, e]) for e in range(el)]
    for c in wloads + vloads:
        c.start()
    pl.semaphore_wait(barrier, 3)

    def blk(rel, s, q):
        return X.at[q, pl.ds(SLOT[rel] * 2 * T + s * T, T), :]

    def relof(d, s):
        return -s % 8 if d == R else s

    def quarter(d, i):
        return i if d == R else nch - 1 - i

    def has(s, i):
        return s <= 3 or i < nch // 2

    def ag(d, s, i):
        q = quarter(d, i)
        return remote(blk(relof(d, s - 1), 0, q), blk(relof(d, s), 0, q), ags.at[d, s - 1, q], agr.at[d, s - 1, q], dev[d])

    def hasm(d, s):
        return s <= 3 or (s == 4 and d == R)

    def agm(d, s):
        return remote(M.at[2 * SLOT[relof(d, s - 1)]], M.at[2 * SLOT[relof(d, s)]], ms.at[d, s - 1], mr.at[d, s - 1], dev[d])

    def sd(rel, q):
        return remote(blk(rel, 0, q), blk(rel, 1, q), ss.at[rel, q], sr.at[rel, q], side)

    def sdm(rel):
        return remote(M.at[2 * SLOT[rel]], M.at[2 * SLOT[rel] + 1], ss.at[rel, nch], sr.at[rel, nch], side)

    sent = []

    def go(c):
        c.start()
        sent.append(c)

    for d in (R, L):
        go(agm(d, 1))
    go(sdm(0))
    for c in xloads:
        c.wait()
    for i in range(nch):
        for d in (R, L):
            go(ag(d, 1, i))
    for i in range(nch):
        go(sd(0, i))

    def advance_meta(s):
        for d in (R, L):
            if hasm(d, s):
                agm(d, s).wait_recv()
                if s < 4 and hasm(d, s + 1):
                    go(agm(d, s + 1))
                go(sdm(relof(d, s)))

    def advance(s, i):
        for d in (R, L):
            ag(d, s, i).wait_recv()
            if s < 4 and has(s + 1, i):
                go(ag(d, s + 1, i))
            go(sd(relof(d, s), quarter(d, i)))

    tr = lax.broadcasted_iota(jnp.int32, (2 * T, 2 * T), 0)
    tc = lax.broadcasted_iota(jnp.int32, (2 * T, 2 * T), 1)
    tri = jnp.where((tr < tc) & (tr // T == tc // T), 1.0, 0.0).astype(BF16)
    lane = lax.broadcasted_iota(jnp.int32, (1, 2 * T), 1)

    def prep(slot):
        m = M[2 * slot] + pltpu.roll(M[2 * slot + 1], T, 1)
        ids, gs = m[:k], m[k:]
        hits, gates = [], []
        for le in range(el):
            eq = ids == (idx * el + le).astype(F32)
            hits.append(jnp.max(jnp.where(eq, 1.0, 0.0), axis=0, keepdims=True))
            gates.append(jnp.sum(jnp.where(eq, gs, 0.0), axis=0, keepdims=True))
        hm = jnp.concatenate(hits + [jnp.zeros((16 - el, 2 * T), F32)], axis=0)
        rank = jnp.dot(hm.astype(BF16), tri, preferred_element_type=F32)
        oh, gg = [], []
        for le in range(el):
            key = jnp.where(hits[le] > 0.0, rank[le:le + 1] + jnp.where(lane >= T, float(caps[le]), 0.0), -1.0)
            hit = lax.broadcasted_iota(jnp.int32, (2 * caps[le], 2 * T), 0).astype(F32) == key
            oh.append(jnp.where(hit, 1.0, 0.0))
            gg.append(jnp.where(hit, gates[le], 0.0))
        OH[slot] = jnp.concatenate(oh, axis=0).astype(BF16)
        gv = jnp.concatenate(gg, axis=0)
        hi = gv.astype(BF16).astype(F32)
        mid = (gv - hi).astype(BF16).astype(F32)
        lo = gv - hi - mid
        GT[slot] = jnp.concatenate([hi, mid, lo], axis=0).T.astype(BF16)

    def preps(lo, n):
        for j in range(n):
            prep(lo + j)

    NEAR = 5
    passes = ((0, NEAR), (NEAR, 8))

    def arrive(g):
        for rel in RELS[passes[g][0]:passes[g][1]]:
            for q in range(nch):
                sd(rel, q).wait_recv()

    def gather(g):
        lo, hi = passes[g]
        nc = hi - lo
        for c in range(nch):
            for i in range(nc):
                v = jnp.dot(OH[lo + i], X[c, (lo + i) * 2 * T:(lo + i + 1) * 2 * T, :], preferred_element_type=F32).astype(BF16)
                for le in range(el):
                    n2 = 2 * caps[le]
                    r0 = nc * offs[le] + i * n2
                    XG[r0:r0 + n2, c * DC:(c + 1) * DC] = v[offs[le]:offs[le] + n2]

    def experts(g, n):
        lo, hi = passes[g]
        nc = hi - lo
        cols = pl.ds(pl.multiple_of(n * NT, NT), NT)
        for e in range(el):
            m = nc * 2 * caps[e]
            src = pl.ds(nc * offs[e], m)
            dst = pl.ds(8 * offs[e] + lo * 2 * caps[e], m)
            xa, xb = XG[src, :KH], XG[src, KH:]
            a = jnp.dot(xa, W[4 * e, :, cols], preferred_element_type=F32) + jnp.dot(xb, W[4 * e + 1, :, cols], preferred_element_type=F32)
            b = jnp.dot(xa, W[4 * e + 2, :, cols], preferred_element_type=F32) + jnp.dot(xb, W[4 * e + 3, :, cols], preferred_element_type=F32)
            U[dst, cols] = (a * jax.nn.sigmoid(a) * b).astype(BF16)

    steps = F // NT

    advance_meta(1)
    advance_meta(2)
    advance(1, 0)
    advance_meta(3)
    advance(1, 1)
    advance_meta(4)
    advance(1, 2)
    for rel in RELS:
        sdm(rel).wait_recv()
    preps(0, 2)
    advance(1, 3)
    preps(2, 2)
    advance(2, 0)
    preps(4, 2)
    advance(2, 1)
    preps(6, 2)
    advance(2, 2)
    advance(2, 3)
    arrive(0)
    gather(0)
    advance(3, 0)
    for c in wloads:
        c.wait()
    for n in range(steps):
        experts(0, n)
        for i in ((1, 2), (3,), (), ())[n % 4] if steps == 4 else (1, 2, 3):
            advance(3, i)
    advance(4, 0)
    advance(4, 1)
    arrive(1)
    gather(1)

    def far(n, _):
        experts(1, n)
        return 0
    lax.fori_loop(0, steps, far, 0)
    w2loads = []
    for c in range(1, nch):
        for e in range(el):
            w2loads.append(pltpu.make_async_copy(w2.at[e, :, pl.ds(c * DC, DC)], W.at[4 * (c // 2) + e, :, pl.ds((c % 2) * DC, DC)], vsem.at[c, e]))
            w2loads[-1].start()
    for c in sent:
        c.wait_send()
    del sent[:]

    def h_rows(slot, lo, n):
        return X.at[slot // 2, pl.ds((slot % 2) * 3 * rows + lo, n), :]

    def d2d(c, part):
        if part == 0:
            return remote(SF.at[c], S.at[c, pl.ds(NEAR, 8 - NEAR)], ds_.at[c, 0], dr.at[c, 0], side)
        return remote(SN.at[c % 2], S.at[c, pl.ds(0, NEAR)], ds_.at[c, 1], dr.at[c, 1], side)

    nt = min(256, DC)

    def tile(c, part):
        lo, hi = passes[1 - part]
        if part == 0:
            for w in vloads if c == 0 else w2loads[4 * c - 4:4 * c]:
                w.wait()
        elif c >= 2:
            d2d(c - 2, 1).wait_send()
        for e in range(el):
            n2 = 2 * caps[e]
            m = (hi - lo) * n2
            for n in range(DC // nt):
                if c == 0:
                    w = V[e, :, n * nt:(n + 1) * nt]
                else:
                    w = W[4 * (c // 2) + e, :, pl.ds((c % 2) * DC + n * nt, nt)]
                h = jnp.dot(U[pl.ds(8 * offs[e] + lo * n2, m), :], w, preferred_element_type=F32).astype(BF16)
                for j in range(hi - lo):
                    for p in range(3):
                        h_rows(lo + j, p * rows + offs[e], n2)[:, n * nt:(n + 1) * nt] = h[j * n2:(j + 1) * n2]
        for slot in range(lo, hi):
            v = jnp.dot(GT[slot], h_rows(slot, 0, 3 * rows)[...], preferred_element_type=F32)
            OWN[c, slot] = v[:T]
            if part == 0:
                SF[c, slot - NEAR] = v[T:]
            else:
                SN[c % 2, slot] = v[T:]
        d2d(c, part).start()

    A, B = slice(0, HC), slice(HC, DC)

    def ring(c, s, d):
        cols = pl.ds(0, DC) if s else pl.ds(d * HC, HC)
        rel = 4 - s if d == R else 4 + s
        return remote(OWN.at[c, SLOT[rel], :, cols], RR.at[c, d, s, :, cols], rs.at[c, d, s], rr.at[c, d, s], dev[d])

    def step(c, s):
        if s == 0:
            d2d(c, 0).wait_recv()
            OWN[c, SLOT[4]] += S[c, SLOT[4]]
        if s == 2:
            d2d(c, 1).wait_recv()
        for d in (R, L):
            if s:
                q = SLOT[4 - s if d == R else 4 + s]
                ring(c, s - 1, d).wait_recv()
                if s == 1:
                    h, o = (A, B) if d == R else (B, A)
                    OWN[c, q, :, h] += S[c, q, :, h] + RR[c, d, 0, :, h]
                    OWN[c, q, :, o] += S[c, q, :, o]
                else:
                    OWN[c, q] += S[c, q] + RR[c, d, s - 1]
            go(ring(c, s, d))

    def final(c):
        for d in (R, L):
            ring(c, 3, d).wait_recv()
        y = OWN[c, 0] + S[c, 0] + (RR[c, R, 3] + RR[c, L, 3])
        out_ref[:, c * DC:(c + 1) * DC] = y.astype(BF16)

    tile(0, 0)
    for c in range(1, nch):
        tile(c, 0)
        step(c - 1, 0)
    step(nch - 1, 0)
    for c in range(nch):
        step(c, 1)
        tile(c, 1)
    for s in (2, 3):
        for c in range(nch):
            step(c, s)
    for c in range(nch):
        final(c)
    for c in sent:
        c.wait_send()
    for c in range(nch):
        d2d(c, 0).wait_send()
    for c in (nch - 2, nch - 1):
        d2d(c, 1).wait_send()


def solution(mesh):
    n = mesh.shape['expert']
    nz = n // 4

    def local(x, idx, g, hot_tok, w1, w3, w2):
        t, d = x.shape
        k = idx.shape[1]
        el, _, f = w1.shape
        e = el * n
        ch = hot_tok.shape[0]
        cap = 2 * ((t * k - ch + e - 2) // (e - 1))
        nch = 4
        dc = d // nch
        rows = 2 * (ch + (el - 1) * cap)
        dma = pltpu.SemaphoreType.DMA
        vmem = pl.BlockSpec(memory_space=pltpu.VMEM)
        hbm = pl.BlockSpec(memory_space=pl.ANY)
        return pl.pallas_call(
            functools.partial(_kernel, nch, ch, cap, nz),
            name='moe',
            out_shape=jax.ShapeDtypeStruct((t, d), BF16),
            in_specs=[hbm, vmem, vmem, hbm, hbm, hbm],
            out_specs=vmem,
            scratch_shapes=[
                pltpu.VMEM((nch, 16 * t, dc), BF16),
                pltpu.VMEM((16, 2 * k, 2 * t), F32),
                pltpu.VMEM((4 * el, d // 2, f), BF16),
                pltpu.VMEM((el, f, dc), BF16),
                pltpu.VMEM((5 * rows, d), BF16),
                pltpu.VMEM((8 * rows, f), BF16),
                pltpu.VMEM((8, rows, 2 * t), BF16),
                pltpu.VMEM((8, 2 * t, 3 * rows), BF16),
                pltpu.VMEM((nch, 8, t, dc), F32),
                pltpu.VMEM((nch, 3, t, dc), F32),
                pltpu.VMEM((2, 5, t, dc), F32),
                pltpu.VMEM((nch, 8, t, dc), F32),
                pltpu.VMEM((nch, 2, 4, t, dc), F32),
                dma((nch,)), dma((4 * el,)), dma((nch, el)),
                dma((2, 4, nch)), dma((2, 4, nch)), dma((2, 4)), dma((2, 4)),
                dma((8, nch + 1)), dma((8, nch + 1)), dma((nch, 2)), dma((nch, 2)),
                dma((nch, 2, 4)), dma((nch, 2, 4)),
            ],
            compiler_params=pltpu.CompilerParams(collective_id=0, has_side_effects=True, vmem_limit_bytes=67043328),
        )(x, idx.T, g.T, w1, w3, w2)

    rows = P(('data', 'expert'))
    wspec = P('expert')
    return jax.shard_map(local, mesh=mesh, in_specs=(rows, rows, rows, rows, wspec, wspec, wspec), out_specs=rows, check_vma=False)
```

```python
import functools

import jax
import jax.numpy as jnp
from jax import lax
from jax.experimental import pallas as pl
from jax.experimental.pallas import tpu as pltpu
from jax.sharding import PartitionSpec as P

F32, BF16 = jnp.float32, jnp.bfloat16
RELS = (0, 1, 7, 2, 6, 3, 5, 4)
SLOT = {r: i for i, r in enumerate(RELS)}
R, L = 0, 1


def _kernel(nch, ch, cap, nz, x_hbm, ids_ref, g_ref, w1, w3, w2, out_ref,
            X, M, W, V, XG, U, OH, GT, OWN, SF, SN, S, RR,
            xs, wsem, vsem, ags, agr, ms, mr, ss, sr, ds_, dr, rs, rr):
    T, D = x_hbm.shape
    el, F = w1.shape[0], w1.shape[2]
    DC = D // nch
    HC = DC // 2
    KH = D // 2
    NT = min(256, F)
    k = ids_ref.shape[0]
    caps = [ch] + [cap] * (el - 1)
    offs = [2 * sum(caps[:i]) for i in range(el)]
    rows = 2 * sum(caps)

    idx = lax.axis_index('expert')
    core = idx % 2
    chip = idx // 2
    cz, cy = chip // 2, chip % 2
    pos = cz * (1 - cy) + (2 * nz - 1 - cz) * cy

    def device(p):
        y = p // nz
        z = p * (1 - y) + (2 * nz - 1 - p) * y
        return (z * 2 + y) * 2 + core

    right = device((pos + 1) % (2 * nz))
    left = device((pos + 2 * nz - 1) % (2 * nz))
    side = chip * 2 + 1 - core
    dev = (right, left)

    def remote(src, dst, s_sem, r_sem, who):
        return pltpu.make_async_remote_copy(src_ref=src, dst_ref=dst, send_sem=s_sem, recv_sem=r_sem,
                                            device_id={'expert': who}, device_id_type=pl.DeviceIdType.MESH)

    xloads = [pltpu.make_async_copy(x_hbm.at[:, pl.ds(c * DC, DC)], X.at[c, pl.ds(0, T), :], xs.at[c]) for c in range(nch)]
    for c in xloads:
        c.start()
    M[0, :, :T] = ids_ref[...].astype(F32)
    M[0, :, T:] = g_ref[...]

    barrier = pltpu.get_barrier_semaphore()
    for who in (right, left, side):
        pl.semaphore_signal(barrier, inc=1, device_id={'expert': who}, device_id_type=pl.DeviceIdType.MESH)
    wloads = []
    for e in range(el):
        for j, w in enumerate((w1, w1, w3, w3)):
            wloads.append(pltpu.make_async_copy(w.at[e, pl.ds((j % 2) * KH, KH), :], W.at[4 * e + j], wsem.at[4 * e + j]))
    vloads = [pltpu.make_async_copy(w2.at[e, :, pl.ds(0, DC)], V.at[e], vsem.at[0, e]) for e in range(el)]
    for c in wloads + vloads:
        c.start()
    pl.semaphore_wait(barrier, 3)

    def blk(rel, s, q):
        return X.at[q, pl.ds(SLOT[rel] * 2 * T + s * T, T), :]

    def relof(d, s):
        return -s % 8 if d == R else s

    def quarter(d, i):
        return i if d == R else nch - 1 - i

    def has(s, i):
        return s <= 3 or i < nch // 2

    def ag(d, s, i):
        q = quarter(d, i)
        return remote(blk(relof(d, s - 1), 0, q), blk(relof(d, s), 0, q), ags.at[d, s - 1, q], agr.at[d, s - 1, q], dev[d])

    def hasm(d, s):
        return s <= 3 or (s == 4 and d == R)

    def agm(d, s):
        return remote(M.at[2 * SLOT[relof(d, s - 1)]], M.at[2 * SLOT[relof(d, s)]], ms.at[d, s - 1], mr.at[d, s - 1], dev[d])

    def sd(rel, q):
        return remote(blk(rel, 0, q), blk(rel, 1, q), ss.at[rel, q], sr.at[rel, q], side)

    def sdm(rel):
        return remote(M.at[2 * SLOT[rel]], M.at[2 * SLOT[rel] + 1], ss.at[rel, nch], sr.at[rel, nch], side)

    sent = []

    def go(c):
        c.start()
        sent.append(c)

    for d in (R, L):
        go(agm(d, 1))
    go(sdm(0))
    for c in xloads:
        c.wait()
    for i in range(nch):
        for d in (R, L):
            go(ag(d, 1, i))
    for i in range(nch):
        go(sd(0, i))

    def advance_meta(s):
        for d in (R, L):
            if hasm(d, s):
                agm(d, s).wait_recv()
                if s < 4 and hasm(d, s + 1):
                    go(agm(d, s + 1))
                go(sdm(relof(d, s)))

    def advance(s, i):
        for d in (R, L):
            ag(d, s, i).wait_recv()
            if s < 4 and has(s + 1, i):
                go(ag(d, s + 1, i))
            go(sd(relof(d, s), quarter(d, i)))

    tr = lax.broadcasted_iota(jnp.int32, (2 * T, 2 * T), 0)
    tc = lax.broadcasted_iota(jnp.int32, (2 * T, 2 * T), 1)
    tri = jnp.where((tr < tc) & (tr // T == tc // T), 1.0, 0.0).astype(BF16)
    lane = lax.broadcasted_iota(jnp.int32, (1, 2 * T), 1)

    def prep(slot):
        mo, mi = M[2 * slot], M[2 * slot + 1]
        ids = jnp.where(lane < T, mo, pltpu.roll(mi, T, 1))
        gs = jnp.where(lane < T, pltpu.roll(mo, T, 1), mi)
        hits, gates = [], []
        for le in range(el):
            eq = ids == (idx * el + le).astype(F32)
            hits.append(jnp.max(jnp.where(eq, 1.0, 0.0), axis=0, keepdims=True))
            gates.append(jnp.sum(jnp.where(eq, gs, 0.0), axis=0, keepdims=True))
        hm = jnp.concatenate(hits + [jnp.zeros((16 - el, 2 * T), F32)], axis=0)
        rank = jnp.dot(hm.astype(BF16), tri, preferred_element_type=F32)
        oh, gg = [], []
        for le in range(el):
            key = jnp.where(hits[le] > 0.0, rank[le:le + 1] + jnp.where(lane >= T, float(caps[le]), 0.0), -1.0)
            hit = lax.broadcasted_iota(jnp.int32, (2 * caps[le], 2 * T), 0).astype(F32) == key
            oh.append(jnp.where(hit, 1.0, 0.0))
            gg.append(jnp.where(hit, gates[le], 0.0))
        OH[slot] = jnp.concatenate(oh, axis=0).astype(BF16)
        gv = jnp.concatenate(gg, axis=0)
        hi = gv.astype(BF16).astype(F32)
        mid = (gv - hi).astype(BF16).astype(F32)
        lo = gv - hi - mid
        GT[slot] = jnp.concatenate([hi, mid, lo], axis=0).T.astype(BF16)

    def tables(*slots):
        for j in slots:
            sdm(RELS[j]).wait_recv()
        for j in slots:
            prep(j)

    NEAR = 5
    passes = ((0, NEAR), (NEAR, 8))

    def gather(g, lo, hi):
        first, last = passes[g]
        nc = last - first
        for rel in RELS[lo:hi]:
            for q in range(nch):
                sd(rel, q).wait_recv()
        for c in range(nch):
            for i in range(lo, hi):
                v = jnp.dot(OH[i], X[c, i * 2 * T:(i + 1) * 2 * T, :], preferred_element_type=F32).astype(BF16)
                for le in range(el):
                    n2 = 2 * caps[le]
                    r0 = nc * offs[le] + (i - first) * n2
                    XG[r0:r0 + n2, c * DC:(c + 1) * DC] = v[offs[le]:offs[le] + n2]

    def experts(g, n):
        lo, hi = passes[g]
        nc = hi - lo
        cols = pl.ds(pl.multiple_of(n * NT, NT), NT)
        for e in range(el):
            m = nc * 2 * caps[e]
            src = pl.ds(nc * offs[e], m)
            dst = pl.ds(8 * offs[e] + lo * 2 * caps[e], m)
            xa, xb = XG[src, :KH], XG[src, KH:]
            a = jnp.dot(xa, W[4 * e, :, cols], preferred_element_type=F32) + jnp.dot(xb, W[4 * e + 1, :, cols], preferred_element_type=F32)
            b = jnp.dot(xa, W[4 * e + 2, :, cols], preferred_element_type=F32) + jnp.dot(xb, W[4 * e + 3, :, cols], preferred_element_type=F32)
            U[dst, cols] = (a * jax.nn.sigmoid(a) * b).astype(BF16)

    steps = F // NT

    tables(0)
    advance_meta(1)
    advance(1, 0)
    advance(1, 1)
    tables(1)
    advance(1, 2)
    tables(2)
    advance(1, 3)
    advance_meta(2)
    advance(2, 0)
    advance(2, 1)
    tables(3)
    advance(2, 2)
    tables(4)
    advance(2, 3)
    advance_meta(3)
    gather(0, 0, NEAR)
    advance(3, 0)
    for c in wloads:
        c.wait()

    def near(n):
        if n < steps:
            experts(0, n)

    near(0)
    advance(3, 1)
    advance(3, 2)
    tables(5, 6)
    near(1)
    advance(3, 3)
    advance_meta(4)
    near(2)
    advance(4, 0)
    tables(7)
    near(3)
    advance(4, 1)
    gather(1, NEAR, 7)
    gather(1, 7, 8)
    for n in range(steps):
        experts(1, n)
    w2loads = []
    for c in range(1, nch):
        for e in range(el):
            w2loads.append(pltpu.make_async_copy(w2.at[e, :, pl.ds(c * DC, DC)], W.at[4 * (c // 2) + e, :, pl.ds((c % 2) * DC, DC)], vsem.at[c, e]))
            w2loads[-1].start()
    for c in sent:
        c.wait_send()
    del sent[:]

    def h_rows(slot, lo, n):
        return X.at[slot // 2, pl.ds((slot % 2) * 3 * rows + lo, n), :]

    def d2d(c, part):
        if part == 0:
            return remote(SF.at[c], S.at[c, pl.ds(NEAR, 8 - NEAR)], ds_.at[c, 0], dr.at[c, 0], side)
        return remote(SN.at[c % 2], S.at[c, pl.ds(0, NEAR)], ds_.at[c, 1], dr.at[c, 1], side)

    nt = min(256, DC)

    def tile(c, part):
        lo, hi = passes[1 - part]
        if part == 0:
            for w in vloads if c == 0 else w2loads[4 * c - 4:4 * c]:
                w.wait()
        elif c >= 2:
            d2d(c - 2, 1).wait_send()
        for e in range(el):
            n2 = 2 * caps[e]
            m = (hi - lo) * n2
            for n in range(DC // nt):
                if c == 0:
                    w = V[e, :, n * nt:(n + 1) * nt]
                else:
                    w = W[4 * (c // 2) + e, :, pl.ds((c % 2) * DC + n * nt, nt)]
                h = jnp.dot(U[pl.ds(8 * offs[e] + lo * n2, m), :], w, preferred_element_type=F32).astype(BF16)
                for j in range(hi - lo):
                    for p in range(3):
                        h_rows(lo + j, p * rows + offs[e], n2)[:, n * nt:(n + 1) * nt] = h[j * n2:(j + 1) * n2]
        for slot in range(lo, hi):
            v = jnp.dot(GT[slot], h_rows(slot, 0, 3 * rows)[...], preferred_element_type=F32)
            OWN[c, slot] = v[:T]
            if part == 0:
                SF[c, slot - NEAR] = v[T:]
            else:
                SN[c % 2, slot] = v[T:]
        d2d(c, part).start()

    A, B = slice(0, HC), slice(HC, DC)

    def ring(c, s, d):
        cols = pl.ds(0, DC) if s else pl.ds(d * HC, HC)
        rel = 4 - s if d == R else 4 + s
        return remote(OWN.at[c, SLOT[rel], :, cols], RR.at[c, d, s, :, cols], rs.at[c, d, s], rr.at[c, d, s], dev[d])

    def step(c, s):
        if s == 0:
            d2d(c, 0).wait_recv()
            OWN[c, SLOT[4]] += S[c, SLOT[4]]
        if s == 2:
            d2d(c, 1).wait_recv()
        for d in (R, L):
            if s:
                q = SLOT[4 - s if d == R else 4 + s]
                ring(c, s - 1, d).wait_recv()
                if s == 1:
                    h, o = (A, B) if d == R else (B, A)
                    OWN[c, q, :, h] += S[c, q, :, h] + RR[c, d, 0, :, h]
                    OWN[c, q, :, o] += S[c, q, :, o]
                else:
                    OWN[c, q] += S[c, q] + RR[c, d, s - 1]
            go(ring(c, s, d))

    def final(c):
        for d in (R, L):
            ring(c, 3, d).wait_recv()
        y = OWN[c, 0] + S[c, 0] + (RR[c, R, 3] + RR[c, L, 3])
        out_ref[:, c * DC:(c + 1) * DC] = y.astype(BF16)

    tile(0, 0)
    for c in range(1, nch):
        tile(c, 0)
        step(c - 1, 0)
    step(nch - 1, 0)
    for c in range(nch):
        step(c, 1)
        tile(c, 1)
    for s in (2, 3):
        for c in range(nch):
            step(c, s)
    for c in range(nch):
        final(c)
    for c in sent:
        c.wait_send()
    for c in range(nch):
        d2d(c, 0).wait_send()
    for c in (nch - 2, nch - 1):
        d2d(c, 1).wait_send()


def solution(mesh):
    n = mesh.shape['expert']
    nz = n // 4

    def local(x, idx, g, hot_tok, w1, w3, w2):
        t, d = x.shape
        k = idx.shape[1]
        el, _, f = w1.shape
        e = el * n
        ch = hot_tok.shape[0]
        cap = 2 * ((t * k - ch + e - 2) // (e - 1))
        nch = 4
        dc = d // nch
        rows = 2 * (ch + (el - 1) * cap)
        dma = pltpu.SemaphoreType.DMA
        vmem = pl.BlockSpec(memory_space=pltpu.VMEM)
        hbm = pl.BlockSpec(memory_space=pl.ANY)
        return pl.pallas_call(
            functools.partial(_kernel, nch, ch, cap, nz),
            name='moe',
            out_shape=jax.ShapeDtypeStruct((t, d), BF16),
            in_specs=[hbm, vmem, vmem, hbm, hbm, hbm],
            out_specs=vmem,
            scratch_shapes=[
                pltpu.VMEM((nch, 16 * t, dc), BF16),
                pltpu.VMEM((16, k, 2 * t), F32),
                pltpu.VMEM((4 * el, d // 2, f), BF16),
                pltpu.VMEM((el, f, dc), BF16),
                pltpu.VMEM((5 * rows, d), BF16),
                pltpu.VMEM((8 * rows, f), BF16),
                pltpu.VMEM((8, rows, 2 * t), BF16),
                pltpu.VMEM((8, 2 * t, 3 * rows), BF16),
                pltpu.VMEM((nch, 8, t, dc), F32),
                pltpu.VMEM((nch, 3, t, dc), F32),
                pltpu.VMEM((2, 5, t, dc), F32),
                pltpu.VMEM((nch, 8, t, dc), F32),
                pltpu.VMEM((nch, 2, 4, t, dc), F32),
                dma((nch,)), dma((4 * el,)), dma((nch, el)),
                dma((2, 4, nch)), dma((2, 4, nch)), dma((2, 4)), dma((2, 4)),
                dma((8, nch + 1)), dma((8, nch + 1)), dma((nch, 2)), dma((nch, 2)),
                dma((nch, 2, 4)), dma((nch, 2, 4)),
            ],
            compiler_params=pltpu.CompilerParams(collective_id=0, has_side_effects=True, vmem_limit_bytes=67043328),
        )(x, idx.T, g.T, w1, w3, w2)

    rows = P(('data', 'expert'))
    wspec = P('expert')
    return jax.shard_map(local, mesh=mesh, in_specs=(rows, rows, rows, rows, wspec, wspec, wspec), out_specs=rows, check_vma=False)
```

```python
import functools

import jax
import jax.numpy as jnp
from jax import lax
from jax.experimental import pallas as pl
from jax.experimental.pallas import tpu as pltpu
from jax.sharding import PartitionSpec as P

F32, BF16 = jnp.float32, jnp.bfloat16
RELS = (0, 1, 7, 2, 6, 3, 5, 4)
SLOT = {r: i for i, r in enumerate(RELS)}
R, L = 0, 1


def _kernel(nch, ch, cap, nz, x_hbm, ids_ref, g_ref, w1, w3, w2, out_ref,
            X, M, W, V, XG, U, OH, GT, OWN, SF, SN, S, RR,
            xs, wsem, vsem, ags, agr, ms, mr, ss, sr, ds_, dr, rs, rr):
    T, D = x_hbm.shape
    el, F = w1.shape[0], w1.shape[2]
    DC = D // nch
    HC = DC // 2
    KH = D // 2
    NT = min(256, F)
    k = ids_ref.shape[0]
    caps = [ch] + [cap] * (el - 1)
    offs = [2 * sum(caps[:i]) for i in range(el)]
    rows = 2 * sum(caps)

    idx = lax.axis_index('expert')
    core = idx % 2
    chip = idx // 2
    cz, cy = chip // 2, chip % 2
    pos = cz * (1 - cy) + (2 * nz - 1 - cz) * cy

    def device(p):
        y = p // nz
        z = p * (1 - y) + (2 * nz - 1 - p) * y
        return (z * 2 + y) * 2 + core

    right = device((pos + 1) % (2 * nz))
    left = device((pos + 2 * nz - 1) % (2 * nz))
    side = chip * 2 + 1 - core
    dev = (right, left)

    def remote(src, dst, s_sem, r_sem, who):
        return pltpu.make_async_remote_copy(src_ref=src, dst_ref=dst, send_sem=s_sem, recv_sem=r_sem,
                                            device_id={'expert': who}, device_id_type=pl.DeviceIdType.MESH)

    xloads = [pltpu.make_async_copy(x_hbm.at[:, pl.ds(c * DC, DC)], X.at[c, pl.ds(0, T), :], xs.at[c]) for c in range(nch)]
    for c in xloads:
        c.start()
    M[0, :, :T] = ids_ref[...].astype(F32)
    M[0, :, T:] = g_ref[...]

    barrier = pltpu.get_barrier_semaphore()
    for who in (right, left, side):
        pl.semaphore_signal(barrier, inc=1, device_id={'expert': who}, device_id_type=pl.DeviceIdType.MESH)
    wloads = []
    for e in range(el):
        for j, w in enumerate((w1, w1, w3, w3)):
            wloads.append(pltpu.make_async_copy(w.at[e, pl.ds((j % 2) * KH, KH), :], W.at[4 * e + j], wsem.at[4 * e + j]))
    vloads = [pltpu.make_async_copy(w2.at[e, :, pl.ds(0, DC)], V.at[e], vsem.at[0, e]) for e in range(el)]
    for c in wloads + vloads:
        c.start()
    pl.semaphore_wait(barrier, 3)

    def blk(rel, s, q):
        return X.at[q, pl.ds(SLOT[rel] * 2 * T + s * T, T), :]

    def relof(d, s):
        return -s % 8 if d == R else s

    def quarter(d, i):
        return i if d == R else nch - 1 - i

    def has(s, i):
        return s <= 3 or i < nch // 2

    def ag(d, s, i):
        q = quarter(d, i)
        return remote(blk(relof(d, s - 1), 0, q), blk(relof(d, s), 0, q), ags.at[d, s - 1, q], agr.at[d, s - 1, q], dev[d])

    def hasm(d, s):
        return s <= 3 or (s == 4 and d == R)

    def agm(d, s):
        return remote(M.at[2 * SLOT[relof(d, s - 1)]], M.at[2 * SLOT[relof(d, s)]], ms.at[d, s - 1], mr.at[d, s - 1], dev[d])

    def sd(rel, q):
        return remote(blk(rel, 0, q), blk(rel, 1, q), ss.at[rel, q], sr.at[rel, q], side)

    def sdm(rel):
        return remote(M.at[2 * SLOT[rel]], M.at[2 * SLOT[rel] + 1], ss.at[rel, nch], sr.at[rel, nch], side)

    sent = []

    def go(c):
        c.start()
        sent.append(c)

    for d in (R, L):
        go(agm(d, 1))
    go(sdm(0))
    for c in xloads:
        c.wait()
    for i in range(nch):
        for d in (R, L):
            go(ag(d, 1, i))
    for i in range(nch):
        go(sd(0, i))

    def advance_meta(s):
        for d in (R, L):
            if hasm(d, s):
                agm(d, s).wait_recv()
                if s < 4 and hasm(d, s + 1):
                    go(agm(d, s + 1))
                go(sdm(relof(d, s)))

    def advance(s, i):
        for d in (R, L):
            ag(d, s, i).wait_recv()
            if s < 4 and has(s + 1, i):
                go(ag(d, s + 1, i))
            go(sd(relof(d, s), quarter(d, i)))

    tr = lax.broadcasted_iota(jnp.int32, (2 * T, 2 * T), 0)
    tc = lax.broadcasted_iota(jnp.int32, (2 * T, 2 * T), 1)
    tri = jnp.where((tr < tc) & (tr // T == tc // T), 1.0, 0.0).astype(BF16)
    lane = lax.broadcasted_iota(jnp.int32, (1, 2 * T), 1)

    def prep(slot):
        mo, mi = M[2 * slot], M[2 * slot + 1]
        ids = jnp.where(lane < T, mo, pltpu.roll(mi, T, 1))
        gs = jnp.where(lane < T, pltpu.roll(mo, T, 1), mi)
        hits, gates = [], []
        for le in range(el):
            eq = ids == (idx * el + le).astype(F32)
            hits.append(jnp.max(jnp.where(eq, 1.0, 0.0), axis=0, keepdims=True))
            gates.append(jnp.sum(jnp.where(eq, gs, 0.0), axis=0, keepdims=True))
        hm = jnp.concatenate(hits + [jnp.zeros((16 - el, 2 * T), F32)], axis=0)
        rank = jnp.dot(hm.astype(BF16), tri, preferred_element_type=F32)
        oh, gg = [], []
        for le in range(el):
            key = jnp.where(hits[le] > 0.0, rank[le:le + 1] + jnp.where(lane >= T, float(caps[le]), 0.0), -1.0)
            hit = lax.broadcasted_iota(jnp.int32, (2 * caps[le], 2 * T), 0).astype(F32) == key
            oh.append(jnp.where(hit, 1.0, 0.0))
            gg.append(jnp.where(hit, gates[le], 0.0))
        OH[slot] = jnp.concatenate(oh, axis=0).astype(BF16)
        gv = jnp.concatenate(gg, axis=0)
        hi = gv.astype(BF16).astype(F32)
        mid = (gv - hi).astype(BF16).astype(F32)
        lo = gv - hi - mid
        GT[slot] = jnp.concatenate([hi, mid, lo], axis=0).T.astype(BF16)

    def tables(*slots):
        for j in slots:
            sdm(RELS[j]).wait_recv()
        for j in slots:
            prep(j)

    NEAR = 5
    passes = ((0, 3), (3, NEAR), (NEAR, 8))
    parts = ((NEAR, 8), (0, NEAR))

    def gather(g, lo, hi):
        first, last = passes[g]
        nc = last - first
        for rel in RELS[lo:hi]:
            for q in range(nch):
                sd(rel, q).wait_recv()
        for c in range(nch):
            for i in range(lo, hi):
                v = jnp.dot(OH[i], X[c, i * 2 * T:(i + 1) * 2 * T, :], preferred_element_type=F32).astype(BF16)
                for le in range(el):
                    n2 = 2 * caps[le]
                    r0 = nc * offs[le] + (i - first) * n2
                    XG[g % 2, r0:r0 + n2, c * DC:(c + 1) * DC] = v[offs[le]:offs[le] + n2]

    def experts(g, n):
        lo, hi = passes[g]
        nc = hi - lo
        cols = pl.ds(pl.multiple_of(n * NT, NT), NT)
        for e in range(el):
            m = nc * 2 * caps[e]
            src = pl.ds(nc * offs[e], m)
            dst = pl.ds(8 * offs[e] + lo * 2 * caps[e], m)
            xa, xb = XG[g % 2, src, :KH], XG[g % 2, src, KH:]
            a = jnp.dot(xa, W[4 * e, :, cols], preferred_element_type=F32) + jnp.dot(xb, W[4 * e + 1, :, cols], preferred_element_type=F32)
            b = jnp.dot(xa, W[4 * e + 2, :, cols], preferred_element_type=F32) + jnp.dot(xb, W[4 * e + 3, :, cols], preferred_element_type=F32)
            U[dst, cols] = (a * jax.nn.sigmoid(a) * b).astype(BF16)

    steps = F // NT

    def body(g, n):
        if n < steps:
            experts(g, n)

    tables(0)
    advance_meta(1)
    advance(1, 0)
    advance(1, 1)
    tables(1)
    advance(1, 2)
    tables(2)
    advance(1, 3)
    advance_meta(2)
    advance(2, 0)
    gather(0, 0, 3)
    for c in wloads:
        c.wait()
    body(0, 0)
    advance(2, 1)
    advance(2, 2)
    tables(3)
    body(0, 1)
    advance(2, 3)
    advance_meta(3)
    tables(4)
    body(0, 2)
    advance(3, 0)
    body(0, 3)
    advance(3, 1)
    gather(1, 3, NEAR)
    body(1, 0)
    advance(3, 2)
    tables(5)
    body(1, 1)
    advance(3, 3)
    advance_meta(4)
    tables(6)
    body(1, 2)
    advance(4, 0)
    tables(7)
    gather(2, NEAR, 7)
    advance(4, 1)
    body(1, 3)
    gather(2, 7, 8)
    for n in range(steps):
        experts(2, n)
    w2loads = []
    for c in range(1, nch):
        for e in range(el):
            w2loads.append(pltpu.make_async_copy(w2.at[e, :, pl.ds(c * DC, DC)], W.at[4 * (c // 2) + e, :, pl.ds((c % 2) * DC, DC)], vsem.at[c, e]))
            w2loads[-1].start()
    for c in sent:
        c.wait_send()
    del sent[:]

    def h_rows(slot, lo, n):
        return X.at[slot // 2, pl.ds((slot % 2) * 3 * rows + lo, n), :]

    def d2d(c, part):
        if part == 0:
            return remote(SF.at[c], S.at[c, pl.ds(NEAR, 8 - NEAR)], ds_.at[c, 0], dr.at[c, 0], side)
        return remote(SN.at[c % 2], S.at[c, pl.ds(0, NEAR)], ds_.at[c, 1], dr.at[c, 1], side)

    nt = min(256, DC)

    def tile(c, part):
        lo, hi = parts[part]
        if part == 0:
            for w in vloads if c == 0 else w2loads[4 * c - 4:4 * c]:
                w.wait()
        elif c >= 2:
            d2d(c - 2, 1).wait_send()
        for e in range(el):
            n2 = 2 * caps[e]
            m = (hi - lo) * n2
            for n in range(DC // nt):
                if c == 0:
                    w = V[e, :, n * nt:(n + 1) * nt]
                else:
                    w = W[4 * (c // 2) + e, :, pl.ds((c % 2) * DC + n * nt, nt)]
                h = jnp.dot(U[pl.ds(8 * offs[e] + lo * n2, m), :], w, preferred_element_type=F32).astype(BF16)
                for j in range(hi - lo):
                    for p in range(3):
                        h_rows(lo + j, p * rows + offs[e], n2)[:, n * nt:(n + 1) * nt] = h[j * n2:(j + 1) * n2]
        for slot in range(lo, hi):
            v = jnp.dot(GT[slot], h_rows(slot, 0, 3 * rows)[...], preferred_element_type=F32)
            OWN[c, slot] = v[:T]
            if part == 0:
                SF[c, slot - NEAR] = v[T:]
            else:
                SN[c % 2, slot] = v[T:]
        d2d(c, part).start()

    A, B = slice(0, HC), slice(HC, DC)

    def ring(c, s, d):
        cols = pl.ds(0, DC) if s else pl.ds(d * HC, HC)
        rel = 4 - s if d == R else 4 + s
        return remote(OWN.at[c, SLOT[rel], :, cols], RR.at[c, d, s, :, cols], rs.at[c, d, s], rr.at[c, d, s], dev[d])

    def step(c, s):
        if s == 0:
            d2d(c, 0).wait_recv()
            OWN[c, SLOT[4]] += S[c, SLOT[4]]
        if s == 2:
            d2d(c, 1).wait_recv()
        for d in (R, L):
            if s:
                q = SLOT[4 - s if d == R else 4 + s]
                ring(c, s - 1, d).wait_recv()
                if s == 1:
                    h, o = (A, B) if d == R else (B, A)
                    OWN[c, q, :, h] += S[c, q, :, h] + RR[c, d, 0, :, h]
                    OWN[c, q, :, o] += S[c, q, :, o]
                else:
                    OWN[c, q] += S[c, q] + RR[c, d, s - 1]
            go(ring(c, s, d))

    def final(c):
        for d in (R, L):
            ring(c, 3, d).wait_recv()
        y = OWN[c, 0] + S[c, 0] + (RR[c, R, 3] + RR[c, L, 3])
        out_ref[:, c * DC:(c + 1) * DC] = y.astype(BF16)

    tile(0, 0)
    for c in range(1, nch):
        tile(c, 0)
        step(c - 1, 0)
    step(nch - 1, 0)
    for c in range(nch):
        step(c, 1)
        tile(c, 1)
    for s in (2, 3):
        for c in range(nch):
            step(c, s)
    for c in range(nch):
        final(c)
    for c in sent:
        c.wait_send()
    for c in range(nch):
        d2d(c, 0).wait_send()
    for c in (nch - 2, nch - 1):
        d2d(c, 1).wait_send()


def solution(mesh):
    n = mesh.shape['expert']
    nz = n // 4

    def local(x, idx, g, hot_tok, w1, w3, w2):
        t, d = x.shape
        k = idx.shape[1]
        el, _, f = w1.shape
        e = el * n
        ch = hot_tok.shape[0]
        cap = 2 * ((t * k - ch + e - 2) // (e - 1))
        nch = 4
        dc = d // nch
        rows = 2 * (ch + (el - 1) * cap)
        dma = pltpu.SemaphoreType.DMA
        vmem = pl.BlockSpec(memory_space=pltpu.VMEM)
        hbm = pl.BlockSpec(memory_space=pl.ANY)
        return pl.pallas_call(
            functools.partial(_kernel, nch, ch, cap, nz),
            name='moe',
            out_shape=jax.ShapeDtypeStruct((t, d), BF16),
            in_specs=[hbm, vmem, vmem, hbm, hbm, hbm],
            out_specs=vmem,
            scratch_shapes=[
                pltpu.VMEM((nch, 16 * t, dc), BF16),
                pltpu.VMEM((16, k, 2 * t), F32),
                pltpu.VMEM((4 * el, d // 2, f), BF16),
                pltpu.VMEM((el, f, dc), BF16),
                pltpu.VMEM((2, 3 * rows, d), BF16),
                pltpu.VMEM((8 * rows, f), BF16),
                pltpu.VMEM((8, rows, 2 * t), BF16),
                pltpu.VMEM((8, 2 * t, 3 * rows), BF16),
                pltpu.VMEM((nch, 8, t, dc), F32),
                pltpu.VMEM((nch, 3, t, dc), F32),
                pltpu.VMEM((2, 5, t, dc), F32),
                pltpu.VMEM((nch, 8, t, dc), F32),
                pltpu.VMEM((nch, 2, 4, t, dc), F32),
                dma((nch,)), dma((4 * el,)), dma((nch, el)),
                dma((2, 4, nch)), dma((2, 4, nch)), dma((2, 4)), dma((2, 4)),
                dma((8, nch + 1)), dma((8, nch + 1)), dma((nch, 2)), dma((nch, 2)),
                dma((nch, 2, 4)), dma((nch, 2, 4)),
            ],
            compiler_params=pltpu.CompilerParams(collective_id=0, has_side_effects=True, vmem_limit_bytes=67043328),
        )(x, idx.T, g.T, w1, w3, w2)

    rows = P(('data', 'expert'))
    wspec = P('expert')
    return jax.shard_map(local, mesh=mesh, in_specs=(rows, rows, rows, rows, wspec, wspec, wspec), out_specs=rows, check_vma=False)
```

```python
import functools

import jax
import jax.numpy as jnp
from jax import lax
from jax.experimental import pallas as pl
from jax.experimental.pallas import tpu as pltpu
from jax.sharding import PartitionSpec as P

F32, BF16 = jnp.float32, jnp.bfloat16
RELS = (0, 1, 7, 2, 6, 3, 5, 4)
SLOT = {r: i for i, r in enumerate(RELS)}
R, L = 0, 1


def _kernel(nch, ch, cap, nz, x_hbm, ids_ref, g_ref, w1, w3, w2, out_ref,
            X, M, W, V, XG, U, OH, GT, OWN, SF, SN, S, RR,
            xs, wsem, vsem, ags, agr, ms, mr, ss, sr, ds_, dr, rs, rr):
    T, D = x_hbm.shape
    el, F = w1.shape[0], w1.shape[2]
    DC = D // nch
    HC = DC // 2
    KH = D // 2
    NT = min(256, F)
    k = ids_ref.shape[0]
    caps = [ch] + [cap] * (el - 1)
    offs = [2 * sum(caps[:i]) for i in range(el)]
    rows = 2 * sum(caps)

    idx = lax.axis_index('expert')
    core = idx % 2
    chip = idx // 2
    cz, cy = chip // 2, chip % 2
    pos = cz * (1 - cy) + (2 * nz - 1 - cz) * cy

    def device(p):
        y = p // nz
        z = p * (1 - y) + (2 * nz - 1 - p) * y
        return (z * 2 + y) * 2 + core

    right = device((pos + 1) % (2 * nz))
    left = device((pos + 2 * nz - 1) % (2 * nz))
    side = chip * 2 + 1 - core
    dev = (right, left)

    def remote(src, dst, s_sem, r_sem, who):
        return pltpu.make_async_remote_copy(src_ref=src, dst_ref=dst, send_sem=s_sem, recv_sem=r_sem,
                                            device_id={'expert': who}, device_id_type=pl.DeviceIdType.MESH)

    barrier = pltpu.get_barrier_semaphore()
    for who in (right, left, side):
        pl.semaphore_signal(barrier, inc=1, device_id={'expert': who}, device_id_type=pl.DeviceIdType.MESH)
    xloads = [pltpu.make_async_copy(x_hbm.at[:, pl.ds(c * DC, DC)], X.at[c, pl.ds(0, T), :], xs.at[c]) for c in range(nch)]
    for c in xloads:
        c.start()
    M[0, :, :T] = ids_ref[...].astype(F32)
    M[0, :, T:] = g_ref[...]

    wloads = []
    for e in range(el):
        for j, w in enumerate((w1, w1, w3, w3)):
            wloads.append(pltpu.make_async_copy(w.at[e, pl.ds((j % 2) * KH, KH), :], W.at[4 * e + j], wsem.at[4 * e + j]))
    vloads = [pltpu.make_async_copy(w2.at[e, :, pl.ds(0, DC)], V.at[e], vsem.at[0, e]) for e in range(el)]
    for c in wloads + vloads:
        c.start()
    pl.semaphore_wait(barrier, 3)

    def blk(rel, s, q):
        return X.at[q, pl.ds(SLOT[rel] * 2 * T + s * T, T), :]

    def relof(d, s):
        return -s % 8 if d == R else s

    def quarter(d, i):
        return i if d == R else nch - 1 - i

    def has(s, i):
        return s <= 3 or i < nch // 2

    def ag(d, s, i):
        q = quarter(d, i)
        return remote(blk(relof(d, s - 1), 0, q), blk(relof(d, s), 0, q), ags.at[d, s - 1, q], agr.at[d, s - 1, q], dev[d])

    def hasm(d, s):
        return s <= 3 or (s == 4 and d == R)

    def agm(d, s):
        return remote(M.at[2 * SLOT[relof(d, s - 1)]], M.at[2 * SLOT[relof(d, s)]], ms.at[d, s - 1], mr.at[d, s - 1], dev[d])

    def sd(rel, q):
        return remote(blk(rel, 0, q), blk(rel, 1, q), ss.at[rel, q], sr.at[rel, q], side)

    def sdm(rel):
        return remote(M.at[2 * SLOT[rel]], M.at[2 * SLOT[rel] + 1], ss.at[rel, nch], sr.at[rel, nch], side)

    sent = []

    def go(c):
        c.start()
        sent.append(c)

    for d in (R, L):
        go(agm(d, 1))
    go(sdm(0))
    for c in xloads:
        c.wait()
    for i in range(nch):
        for d in (R, L):
            go(ag(d, 1, i))
    for i in range(nch):
        go(sd(0, i))

    def advance_meta(s):
        for d in (R, L):
            if hasm(d, s):
                agm(d, s).wait_recv()
                if s < 4 and hasm(d, s + 1):
                    go(agm(d, s + 1))
                go(sdm(relof(d, s)))

    def advance(s, i):
        for d in (R, L):
            ag(d, s, i).wait_recv()
            if s < 4 and has(s + 1, i):
                go(ag(d, s + 1, i))
            go(sd(relof(d, s), quarter(d, i)))

    tr = lax.broadcasted_iota(jnp.int32, (2 * T, 2 * T), 0)
    tc = lax.broadcasted_iota(jnp.int32, (2 * T, 2 * T), 1)
    tri = jnp.where((tr < tc) & (tr // T == tc // T), 1.0, 0.0).astype(BF16)
    lane = lax.broadcasted_iota(jnp.int32, (1, 2 * T), 1)

    def prep(slot):
        mo, mi = M[2 * slot], M[2 * slot + 1]
        ids = jnp.where(lane < T, mo, pltpu.roll(mi, T, 1))
        gs = jnp.where(lane < T, pltpu.roll(mo, T, 1), mi)
        hits, gates = [], []
        for le in range(el):
            eq = ids == (idx * el + le).astype(F32)
            hits.append(jnp.max(jnp.where(eq, 1.0, 0.0), axis=0, keepdims=True))
            gates.append(jnp.sum(jnp.where(eq, gs, 0.0), axis=0, keepdims=True))
        hm = jnp.concatenate(hits + [jnp.zeros((16 - el, 2 * T), F32)], axis=0)
        rank = jnp.dot(hm.astype(BF16), tri, preferred_element_type=F32)
        oh, gg = [], []
        for le in range(el):
            key = jnp.where(hits[le] > 0.0, rank[le:le + 1] + jnp.where(lane >= T, float(caps[le]), 0.0), -1.0)
            hit = lax.broadcasted_iota(jnp.int32, (2 * caps[le], 2 * T), 0).astype(F32) == key
            oh.append(jnp.where(hit, 1.0, 0.0))
            gg.append(jnp.where(hit, gates[le], 0.0))
        OH[slot] = jnp.concatenate(oh, axis=0).astype(BF16)
        gv = jnp.concatenate(gg, axis=0)
        hi = gv.astype(BF16).astype(F32)
        mid = (gv - hi).astype(BF16).astype(F32)
        lo = gv - hi - mid
        GT[slot] = jnp.concatenate([hi, mid, lo], axis=0).T.astype(BF16)

    def tables(*slots):
        for j in slots:
            sdm(RELS[j]).wait_recv()
        for j in slots:
            prep(j)

    NEAR = 5
    passes = ((0, 3), (3, NEAR), (NEAR, 8))
    parts = ((NEAR, 8), (0, NEAR))

    def gather(g, lo, hi):
        first, last = passes[g]
        nc = last - first
        for rel in RELS[lo:hi]:
            for q in range(nch):
                sd(rel, q).wait_recv()
        for c in range(nch):
            for i in range(lo, hi):
                v = jnp.dot(OH[i], X[c, i * 2 * T:(i + 1) * 2 * T, :], preferred_element_type=F32).astype(BF16)
                for le in range(el):
                    n2 = 2 * caps[le]
                    r0 = nc * offs[le] + (i - first) * n2
                    XG[g % 2, r0:r0 + n2, c * DC:(c + 1) * DC] = v[offs[le]:offs[le] + n2]

    def experts(g, n):
        lo, hi = passes[g]
        nc = hi - lo
        cols = pl.ds(pl.multiple_of(n * NT, NT), NT)
        for e in range(el):
            m = nc * 2 * caps[e]
            src = pl.ds(nc * offs[e], m)
            dst = pl.ds(8 * offs[e] + lo * 2 * caps[e], m)
            xa, xb = XG[g % 2, src, :KH], XG[g % 2, src, KH:]
            a = jnp.dot(xa, W[4 * e, :, cols], preferred_element_type=F32) + jnp.dot(xb, W[4 * e + 1, :, cols], preferred_element_type=F32)
            b = jnp.dot(xa, W[4 * e + 2, :, cols], preferred_element_type=F32) + jnp.dot(xb, W[4 * e + 3, :, cols], preferred_element_type=F32)
            U[dst, cols] = (a * jax.nn.sigmoid(a) * b).astype(BF16)

    steps = F // NT

    def body(g, n):
        if n < steps:
            experts(g, n)

    tables(0)
    advance_meta(1)
    advance(1, 0)
    advance(1, 1)
    tables(1)
    advance(1, 2)
    tables(2)
    advance(1, 3)
    advance_meta(2)
    advance(2, 0)
    gather(0, 0, 3)
    for c in wloads:
        c.wait()
    body(0, 0)
    advance(2, 1)
    advance(2, 2)
    tables(3)
    body(0, 1)
    advance(2, 3)
    advance_meta(3)
    tables(4)
    body(0, 2)
    advance(3, 0)
    body(0, 3)
    advance(3, 1)
    gather(1, 3, NEAR)
    body(1, 0)
    advance(3, 2)
    tables(5)
    body(1, 1)
    advance(3, 3)
    advance_meta(4)
    tables(6)
    body(1, 2)
    advance(4, 0)
    tables(7)
    gather(2, NEAR, 7)
    advance(4, 1)
    body(1, 3)
    gather(2, 7, 8)
    for n in range(steps):
        experts(2, n)
    w2loads = []
    for c in range(1, nch):
        for e in range(el):
            w2loads.append(pltpu.make_async_copy(w2.at[e, :, pl.ds(c * DC, DC)], W.at[4 * (c // 2) + e, :, pl.ds((c % 2) * DC, DC)], vsem.at[c, e]))
            w2loads[-1].start()
    for c in sent:
        c.wait_send()
    del sent[:]

    def h_rows(slot, lo, n):
        return X.at[slot // 2, pl.ds((slot % 2) * 3 * rows + lo, n), :]

    def d2d(c, part):
        if part == 0:
            return remote(SF.at[c], S.at[c, pl.ds(NEAR, 8 - NEAR)], ds_.at[c, 0], dr.at[c, 0], side)
        return remote(SN.at[c % 2], S.at[c, pl.ds(0, NEAR)], ds_.at[c, 1], dr.at[c, 1], side)

    nt = min(256, DC)

    def tile(c, part):
        lo, hi = parts[part]
        if part == 0:
            for w in vloads if c == 0 else w2loads[4 * c - 4:4 * c]:
                w.wait()
        elif c >= 2:
            d2d(c - 2, 1).wait_send()
        for e in range(el):
            n2 = 2 * caps[e]
            m = (hi - lo) * n2
            for n in range(DC // nt):
                if c == 0:
                    w = V[e, :, n * nt:(n + 1) * nt]
                else:
                    w = W[4 * (c // 2) + e, :, pl.ds((c % 2) * DC + n * nt, nt)]
                h = jnp.dot(U[pl.ds(8 * offs[e] + lo * n2, m), :], w, preferred_element_type=F32).astype(BF16)
                for j in range(hi - lo):
                    for p in range(3):
                        h_rows(lo + j, p * rows + offs[e], n2)[:, n * nt:(n + 1) * nt] = h[j * n2:(j + 1) * n2]
        for slot in range(lo, hi):
            v = jnp.dot(GT[slot], h_rows(slot, 0, 3 * rows)[...], preferred_element_type=F32)
            OWN[c, slot] = v[:T]
            if part == 0:
                SF[c, slot - NEAR] = v[T:]
            else:
                SN[c % 2, slot] = v[T:]
        d2d(c, part).start()

    A, B = slice(0, HC), slice(HC, DC)

    def ring(c, s, d):
        cols = pl.ds(0, DC) if s else pl.ds(d * HC, HC)
        rel = 4 - s if d == R else 4 + s
        return remote(OWN.at[c, SLOT[rel], :, cols], RR.at[c, d, s, :, cols], rs.at[c, d, s], rr.at[c, d, s], dev[d])

    def step(c, s):
        if s == 0:
            d2d(c, 0).wait_recv()
            OWN[c, SLOT[4]] += S[c, SLOT[4]]
        if s == 2:
            d2d(c, 1).wait_recv()
        for d in (R, L):
            if s:
                q = SLOT[4 - s if d == R else 4 + s]
                ring(c, s - 1, d).wait_recv()
                if s == 1:
                    h, o = (A, B) if d == R else (B, A)
                    OWN[c, q, :, h] += S[c, q, :, h] + RR[c, d, 0, :, h]
                    OWN[c, q, :, o] += S[c, q, :, o]
                else:
                    OWN[c, q] += S[c, q] + RR[c, d, s - 1]
            go(ring(c, s, d))

    def final(c):
        for d in (R, L):
            ring(c, 3, d).wait_recv()
        y = OWN[c, 0] + S[c, 0] + (RR[c, R, 3] + RR[c, L, 3])
        out_ref[:, c * DC:(c + 1) * DC] = y.astype(BF16)

    tile(0, 0)
    for c in range(1, nch):
        tile(c, 0)
        step(c - 1, 0)
    step(nch - 1, 0)
    for c in range(nch):
        step(c, 1)
        tile(c, 1)
    for s in (2, 3):
        for c in range(nch):
            step(c, s)
    for c in range(nch):
        final(c)
    for c in sent:
        c.wait_send()
    for c in range(nch):
        d2d(c, 0).wait_send()
    for c in (nch - 2, nch - 1):
        d2d(c, 1).wait_send()


def solution(mesh):
    n = mesh.shape['expert']
    nz = n // 4

    def local(x, idx, g, hot_tok, w1, w3, w2):
        t, d = x.shape
        k = idx.shape[1]
        el, _, f = w1.shape
        e = el * n
        ch = hot_tok.shape[0]
        cap = 2 * ((t * k - ch + e - 2) // (e - 1))
        nch = 4
        dc = d // nch
        rows = 2 * (ch + (el - 1) * cap)
        dma = pltpu.SemaphoreType.DMA
        vmem = pl.BlockSpec(memory_space=pltpu.VMEM)
        hbm = pl.BlockSpec(memory_space=pl.ANY)
        return pl.pallas_call(
            functools.partial(_kernel, nch, ch, cap, nz),
            name='moe',
            out_shape=jax.ShapeDtypeStruct((t, d), BF16),
            in_specs=[hbm, vmem, vmem, hbm, hbm, hbm],
            out_specs=vmem,
            scratch_shapes=[
                pltpu.VMEM((nch, 16 * t, dc), BF16),
                pltpu.VMEM((16, k, 2 * t), F32),
                pltpu.VMEM((4 * el, d // 2, f), BF16),
                pltpu.VMEM((el, f, dc), BF16),
                pltpu.VMEM((2, 3 * rows, d), BF16),
                pltpu.VMEM((8 * rows, f), BF16),
                pltpu.VMEM((8, rows, 2 * t), BF16),
                pltpu.VMEM((8, 2 * t, 3 * rows), BF16),
                pltpu.VMEM((nch, 8, t, dc), F32),
                pltpu.VMEM((nch, 3, t, dc), F32),
                pltpu.VMEM((2, 5, t, dc), F32),
                pltpu.VMEM((nch, 8, t, dc), F32),
                pltpu.VMEM((nch, 2, 4, t, dc), F32),
                dma((nch,)), dma((4 * el,)), dma((nch, el)),
                dma((2, 4, nch)), dma((2, 4, nch)), dma((2, 4)), dma((2, 4)),
                dma((8, nch + 1)), dma((8, nch + 1)), dma((nch, 2)), dma((nch, 2)),
                dma((nch, 2, 4)), dma((nch, 2, 4)),
            ],
            compiler_params=pltpu.CompilerParams(collective_id=0, has_side_effects=True, vmem_limit_bytes=67043328),
        )(x, idx.T, g.T, w1, w3, w2)

    rows = P(('data', 'expert'))
    wspec = P('expert')
    return jax.shard_map(local, mesh=mesh, in_specs=(rows, rows, rows, rows, wspec, wspec, wspec), out_specs=rows, check_vma=False)
```
